32 devices in a mesh: ma: 8 (over z, x), band: 4 (over y, core).
Axes of the slice: x: 2, y: 2, z: 4, core: 2. Of those that a mesh axis runs over, the one named last changes fastest.
Arguments:
- observed: bfloat16 [256, 64, 1024], P(('ma', 'band')), may hold values from -6 to 6
- eigenvalues: float32 [256, 1024], P(('ma', 'band')), may hold values from 0.05 to 20
- kl_basis: bfloat16 [256, 1024, 512], P(('ma', 'band')), may hold values from -0.1875 to 0.1875
- band_deriv: bfloat16 [40, 512, 512], P('band'), may hold values from -0.15625 to 0.15625, as said below
- counts: int32 [256], P(('ma', 'band')), may hold values from 128 to 1024, as said below
Outputs:
- mode_power: float32 [256, 40], P('ma', 'band')
- band_power: float32 [40], P('band')
The draws below stay inside these ranges and needn't reach their ends.
Inputs may be any that keep to these rules, and one draw needn't show every extreme that they name: counts[m] is the number of leading KL modes of m-mode m that are kept; some m-mode keeps 1024 and some keeps 1024 // 8. Each band_deriv[a] is symmetric.
All inputs are finite; a program needn't handle non-finite values.
Results may differ from the reference program's by a relative error of at most 0.0018.
Values may be sent and summed in bfloat16 or wider, within the bound.
No kernel may reach another device: no remote copies, remote signals or barrier semaphores. Data moves between devices by JAX's collectives and lax.ppermute only.
A program may use at most 64 MiB of HBM per device.

```python
import math
import jax
import jax.numpy as jnp
from jax import lax

BANDS = 40
W = 512
NMAX = 1024
S = 64
MTOT = 256


def draw_band_deriv(key, part):
    gains = jnp.exp(jax.random.uniform(jax.random.fold_in(key, 11), (BANDS, W), jnp.float32, jnp.log(0.5), jnp.log(2.0)))
    raw = jax.random.normal(jax.random.fold_in(key, 12), (BANDS, W, W), jnp.float32)
    rough = jnp.clip((raw + jnp.transpose(raw, (0, 2, 1))) * 0.7071, -4.0, 4.0)
    identity = jnp.eye(W, dtype=jnp.float32)
    matrices = identity[None, :, :] * gains[:, :, None] + 1.5 * rough
    return (matrices * (4.0 / W)).astype(jnp.bfloat16)


def draw_counts(key, part):
    floor_count = NMAX // 8
    values = jax.random.randint(jax.random.fold_in(key, 21), (MTOT,), floor_count, NMAX + 1)
    first_slot = jax.random.randint(jax.random.fold_in(key, 22), (), 0, MTOT)
    second_slot = (first_slot + jax.random.randint(jax.random.fold_in(key, 23), (), 1, MTOT)) % MTOT
    values = values.at[first_slot].set(NMAX).at[second_slot].set(floor_count)
    return values.astype(jnp.int32)


def levels(key, dims, split, smallest, largest):
    gain, own = 1.0, jax.random.fold_in(key, 6)
    for axis_at, parts in split:
        draws = jnp.exp(jax.random.uniform(jax.random.fold_in(own, axis_at), (parts,), jnp.float32, smallest / len(split), largest / len(split)))
        gain = gain * jnp.repeat(draws, dims[axis_at] // parts).reshape([-1 if axis == axis_at else 1 for axis in range(len(dims))])
    return gain


def normal_values(own_key, dims, width, most, shards=(), kind=jnp.bfloat16):
    drawn = jax.random.normal(own_key, dims, jnp.float32) * width
    if len(shards) > 0:
        drawn = levels(own_key, dims, shards, -0.22, 0.18) * drawn
    return jnp.clip(drawn, min=-most, max=most).astype(kind)


def setup_inputs(seed: int = 0) -> dict:
    streams_of = jax.random.split(jax.random.key(seed), 6)
    observed = normal_values(streams_of[0], (MTOT, S, NMAX), 1.0, 6.0, ((0, 32),))
    eigenvalues = jnp.clip(jnp.exp(math.log(20.0) - 5.9914645 * jax.random.uniform(streams_of[1], (MTOT, NMAX), jnp.float32) ** levels(streams_of[1], (MTOT, NMAX), ((0, 32),), -0.2, 0.2)), 0.05, 20.0)
    kl_basis = normal_values(streams_of[2], (MTOT, NMAX, W), NMAX ** -0.5, 0.1875, ((0, 32),))
    band_deriv = draw_band_deriv(jax.random.fold_in(streams_of[5], 71), 0)
    counts = draw_counts(jax.random.fold_in(streams_of[5], 71), 0)
    return {"observed": observed, "eigenvalues": eigenvalues, "kl_basis": kl_basis, "band_deriv": band_deriv, "counts": counts}


def reference(observed, eigenvalues, kl_basis, band_deriv, counts):
    position = lax.broadcasted_iota(jnp.int32, eigenvalues.shape, 1)
    inside = position < counts[:, None]
    weights = jnp.where(inside, 1.0 / (1.0 + eigenvalues), jnp.zeros_like(eigenvalues))
    weighted = (observed.astype(jnp.float32) * weights[:, None, :]).astype(jnp.bfloat16)

    def project_one(operands):
        rows_block, basis_block = operands
        return jnp.dot(rows_block.astype(jnp.float32), basis_block.astype(jnp.float32)).astype(jnp.bfloat16)

    projected = lax.map(project_one, (weighted, kl_basis))
    flattened = projected.astype(jnp.float32).reshape(MTOT * S, W)

    def one_band(matrix):
        mapped = jnp.dot(flattened, matrix.astype(jnp.float32))
        return jnp.sum((mapped * flattened).reshape(MTOT, -1), axis=1)

    quadratic = lax.map(one_band, band_deriv)
    mode_power = jnp.transpose(quadratic) / S
    live_total = jnp.sum(counts).astype(jnp.float32)
    band_power = NMAX * jnp.sum(mode_power, axis=0) / live_total
    return mode_power, band_power
```

```python
import functools

import jax
import jax.numpy as jnp
from jax import lax
from jax.experimental import pallas as pl
from jax.experimental.pallas import tpu as pltpu
from jax.sharding import PartitionSpec as P

DEPTH = 256
EXTRA = 16
BASE = 128
DIGITS = 3
LANES = 128


def project_kernel(first, counts, eigenvalues, observed, basis, out, held, rows, weighted, row_sem, held_sem):
    modes, samples, depth = rows.shape
    steps = depth // DEPTH

    def row_copy(m):
        return pltpu.make_async_copy(observed.at[first + m], rows.at[m], row_sem.at[m])

    def held_copy(m, k):
        part = pl.ds(k * DEPTH, DEPTH)
        return pltpu.make_async_copy(basis.at[first + m, part, :], held.at[m, k], held_sem.at[m, k])

    for m in range(modes):
        row_copy(m).start()
        for k in range(steps):

            @pl.when(k * DEPTH < counts[first + m])
            def _():
                held_copy(m, k).start()

    for m in range(modes):
        count = counts[first + m]
        row_copy(m).wait()
        values = eigenvalues[first + m : first + m + 1, :]
        position = lax.broadcasted_iota(jnp.int32, values.shape, 1)
        weights = jnp.where(position < count, 1.0 / (1.0 + values), jnp.zeros_like(values))
        scaled = (rows[m].astype(jnp.float32) * weights).astype(jnp.bfloat16)
        for k in range(steps):
            weighted[k] = scaled[:, k * DEPTH : (k + 1) * DEPTH]

        def step(k, total):
            held_copy(m, k).wait()
            return total + jnp.dot(weighted[k], held[m, k], preferred_element_type=jnp.float32)

        total = jnp.zeros((samples, out.shape[1]), jnp.float32)
        total = lax.fori_loop(0, (count + DEPTH - 1) // DEPTH, step, total)
        out[m * samples : (m + 1) * samples, :] = total.astype(jnp.bfloat16)

    live = counts[0]
    for m in range(1, counts.shape[0]):
        live = live + counts[m]
    row = lax.broadcasted_iota(jnp.int32, (EXTRA, out.shape[1]), 0)
    digits = jnp.zeros(row.shape, jnp.float32)
    for d in range(DIGITS):
        digit = lax.rem(lax.div(live, BASE**d), BASE)
        digits = jnp.where(row == d, digit.astype(jnp.float32), digits)
    out[modes * samples :, :] = digits.astype(jnp.bfloat16)


def project(first, modes, observed, eigenvalues, kl_basis, counts):
    _, samples, depth = observed.shape
    width = kl_basis.shape[2]
    steps = depth // DEPTH
    return pl.pallas_call(
        functools.partial(project_kernel, first),
        out_shape=jax.ShapeDtypeStruct((modes * samples + EXTRA, width), jnp.bfloat16),
        in_specs=[
            pl.BlockSpec(memory_space=pltpu.SMEM),
            pl.BlockSpec(memory_space=pltpu.VMEM),
            pl.BlockSpec(memory_space=pl.ANY),
            pl.BlockSpec(memory_space=pl.ANY),
        ],
        out_specs=pl.BlockSpec(memory_space=pltpu.VMEM),
        scratch_shapes=[
            pltpu.VMEM((modes, steps, DEPTH, width), jnp.bfloat16),
            pltpu.VMEM((modes, samples, depth), jnp.bfloat16),
            pltpu.VMEM((steps, samples, DEPTH), jnp.bfloat16),
            pltpu.SemaphoreType.DMA((modes,)),
            pltpu.SemaphoreType.DMA((modes, steps)),
        ],
        compiler_params=pltpu.CompilerParams(vmem_limit_bytes=16 * 2**20),
        cost_estimate=pl.CostEstimate(
            flops=2 * modes * samples * depth * width,
            bytes_accessed=2 * modes * depth * (width + samples),
            transcendentals=0,
        ),
        name="project",
    )(counts, eigenvalues, observed, kl_basis)


def quadratic_kernel(sizes, samples, counted, matrices, *refs):
    blocks, out, doubled, wide = refs[: len(sizes)], refs[len(sizes)], refs[-2], refs[-1]
    bands, width, _ = matrices.shape
    half = width // 2
    starts = [sum(sizes[:b]) for b in range(len(sizes))]
    for block, modes, start in zip(blocks, sizes, starts):
        rows = slice(start * samples, (start + modes) * samples)
        left = block[: modes * samples, :half]
        right = block[: modes * samples, half:]
        doubled[rows, :half] = left + left
        doubled[rows, half:] = right
        wide[rows, :half] = left.astype(jnp.float32)
        wide[rows, half:] = right.astype(jnp.float32)

    lane = lax.broadcasted_iota(jnp.int32, (1, LANES), 1)

    def band(a, results):
        updated = []
        for block, modes, start, result in zip(blocks, sizes, starts, results):
            rows = slice(start * samples, (start + modes) * samples)
            first = jnp.dot(
                block[: modes * samples, :half], matrices[a, :half, :half], preferred_element_type=jnp.float32
            )
            second = jnp.dot(doubled[rows, :], matrices[a, :, half:], preferred_element_type=jnp.float32)
            terms = first * wide[rows, :half] + second * wide[rows, half:]
            folded = terms[:, :LANES]
            for k in range(1, half // LANES):
                folded = folded + terms[:, k * LANES : (k + 1) * LANES]
            power = jnp.sum(jnp.sum(folded.reshape(modes, samples, LANES), axis=1), axis=1, keepdims=True)
            updated.append(jnp.where(lane == a, power / samples, result))
        return tuple(updated)

    results = tuple(jnp.zeros((modes, LANES), jnp.float32) for modes in sizes)
    results = lax.fori_loop(0, bands, band, results)
    for b, (block, modes, start, result) in enumerate(zip(blocks, sizes, starts, results)):
        if b in counted:
            digits = block[modes * samples :, :LANES].astype(jnp.float32)
            live = digits[0:1, :]
            for d in range(1, DIGITS):
                live = live + float(BASE**d) * digits[d : d + 1, :]
            mode = lax.broadcasted_iota(jnp.int32, (modes, LANES), 0)
            result = jnp.where((mode == 0) & (lane == bands), live, result)
        out[start : start + modes, :] = result


def quadratic(blocks, samples, counted, matrices):
    bands, width, _ = matrices.shape
    sizes = tuple((block.shape[0] - EXTRA) // samples for block in blocks)
    modes = sum(sizes)
    return pl.pallas_call(
        functools.partial(quadratic_kernel, sizes, samples, counted),
        out_shape=jax.ShapeDtypeStruct((modes, LANES), jnp.float32),
        in_specs=[pl.BlockSpec(memory_space=pltpu.VMEM)] * (1 + len(blocks)),
        out_specs=pl.BlockSpec(memory_space=pltpu.VMEM),
        scratch_shapes=[
            pltpu.VMEM((modes * samples, width), jnp.bfloat16),
            pltpu.VMEM((modes * samples, width), jnp.float32),
        ],
        compiler_params=pltpu.CompilerParams(vmem_limit_bytes=24 * 2**20),
        cost_estimate=pl.CostEstimate(
            flops=2 * bands * modes * samples * width * width,
            bytes_accessed=2 * modes * samples * width,
            transcendentals=0,
        ),
        name="quadratic",
    )(matrices, *blocks)


def collect_kernel(groups, chunk_sizes, bands, *refs):
    results, power, sums, ordered = refs[: len(groups)], refs[-3], refs[-2], refs[-1]
    me = lax.axis_index("band")
    total = sum(chunk_sizes)
    for result, entries in zip(results, groups):
        at = 0
        for offset, chunk in entries:
            modes = chunk_sizes[chunk]
            place = lax.bitwise_xor(me, offset) * total + sum(chunk_sizes[:chunk])
            ordered[pl.ds(place, modes), :] = result[at : at + modes, :]
            at += modes
    values = ordered[...]
    power[...] = jnp.transpose(values)[:bands, :]
    sums[...] = jnp.sum(values, axis=0, keepdims=True)


def collect(results, groups, chunk_sizes, bands, blocks):
    modes = sum(chunk_sizes) * blocks
    return pl.pallas_call(
        functools.partial(collect_kernel, groups, chunk_sizes, bands),
        out_shape=(
            jax.ShapeDtypeStruct((bands, modes), jnp.float32),
            jax.ShapeDtypeStruct((1, LANES), jnp.float32),
        ),
        in_specs=[pl.BlockSpec(memory_space=pltpu.VMEM)] * len(results),
        out_specs=(pl.BlockSpec(memory_space=pltpu.VMEM),) * 2,
        scratch_shapes=[pltpu.VMEM((modes, LANES), jnp.float32)],
        name="collect",
    )(*results)


def normalize_kernel(bands, scale, mine, other, out):
    total = mine[...] + other[...]
    out[...] = scale * total[:, :bands] / total[:, bands : bands + 1]


def per_device(ma, band, observed, eigenvalues, kl_basis, band_deriv, counts):
    own_modes, samples, depth = observed.shape
    bands = band_deriv.shape[0]
    chunk_sizes = (own_modes // 2, own_modes - own_modes // 2)
    last = len(chunk_sizes) - 1

    def swap(array, axis, size, bit):
        return lax.ppermute(array, axis, [(i, i ^ bit) for i in range(size)])

    held = {}
    first = 0
    for c, modes in enumerate(chunk_sizes):
        held[0, c] = project(first, modes, observed, eigenvalues, kl_basis, counts)
        first += modes
    bits = []
    bit = band // 2
    while bit:
        bits.append(bit)
        bit //= 2

    known = [0]
    far = bits[0]
    for c in range(len(chunk_sizes)):
        held[far, c] = swap(held[0, c], "band", band, far)
    near = [0]
    for bit in bits[1:]:
        for offset in list(near):
            for c in range(len(chunk_sizes)):
                held[offset ^ bit, c] = swap(held[offset, c], "band", band, bit)
            near.append(offset ^ bit)
    for c in range(len(chunk_sizes)):
        arrived = [far]
        for bit in bits[1:]:
            for offset in list(arrived):
                held[offset ^ bit, c] = swap(held[offset, c], "band", band, bit)
                arrived.append(offset ^ bit)

    groups = [tuple((offset, c) for offset in near for c in range(len(chunk_sizes)))]
    for c in range(len(chunk_sizes)):
        for offset in near:
            groups.append(((offset ^ far, c),))
    results = []
    for entries in groups:
        counted = tuple(e for e, (_, c) in enumerate(entries) if c == last)
        results.append(quadratic([held[entry] for entry in entries], samples, counted, band_deriv))
    power, sums = collect(results, tuple(groups), chunk_sizes, bands, band)

    bit = 1
    while bit < ma:
        other = swap(sums, "ma", ma, bit)
        if 2 * bit < ma:
            sums = sums + other
        bit *= 2
    total = pl.pallas_call(
        functools.partial(normalize_kernel, bands, float(depth)),
        out_shape=jax.ShapeDtypeStruct((1, bands), jnp.float32),
        name="normalize",
    )(sums, other)
    return jnp.transpose(power), total.reshape(bands)


def solution(mesh):
    in_specs = (
        P(("ma", "band"), None, None),
        P(("ma", "band"), None),
        P(("ma", "band"), None, None),
        P("band", None, None),
        P(("ma", "band")),
    )
    out_specs = (P("ma", "band"), P("band"))
    body = functools.partial(per_device, mesh.shape["ma"], mesh.shape["band"])
    return jax.shard_map(body, mesh=mesh, in_specs=in_specs, out_specs=out_specs, check_vma=False)
```
